32 devices in a mesh: dp: 4 (over x, core), ep: 8 (over z, y).
Axes of the slice: x: 2, y: 2, z: 4, core: 2. Of those that a mesh axis runs over, the one named last changes fastest.
Arguments:
- tokens: bfloat16 [4096, 2048], P(('dp', 'ep')), parts along dimension 0, may hold values from -6 to 6
- expert_ids: int32 [4096, 8], P(('dp', 'ep')), parts along dimension 0, may hold values from 0 to 15, all different within a row; in each aligned block of 32 rows (0 to 31, 32 to 63, ...) at most 32 rows name the same one
- gate_nums: int32 [4096, 8], P(('dp', 'ep')), parts along dimension 0, may hold values from 64 to 1023
- w_gate: bfloat16 [16, 2048, 768], P('ep'), may hold values from -0.125 to 0.125
- w_up: bfloat16 [16, 2048, 768], P('ep'), may hold values from -0.125 to 0.125
- w_down: bfloat16 [16, 768, 2048], P('ep'), may hold values from -0.21875 to 0.21875
Outputs:
- mixed: bfloat16 [4096, 2048], P(('dp', 'ep')), parts along dimension 0
The draws below stay inside these ranges and needn't reach their ends.
There are 4 independent parts, one for each index of `dp`. The reference program is written for one: setup_inputs(seed, part) draws one part's arguments, and reference() takes and returns one part's arrays. A program takes and returns all parts, laid end to end along the dimension named above; an argument that names none is the same for every part. Nothing has to cross between parts.
Inputs may be any that keep to these rules, and one draw needn't show every extreme that they name: `expert_ids`: each row names 8 different experts. In every aligned block of 32 rows no expert is named by more than 32 rows, a bound that some block reaches.
All inputs are finite; a program needn't handle non-finite values.
Results may differ from the reference program's by a relative error of at most 0.008.
Values may be sent and summed in bfloat16 or wider, within the bound.
No kernel may reach another device: no remote copies, remote signals or barrier semaphores. Data moves between devices by JAX's collectives and lax.ppermute only.
A program may use at most 128 MiB of HBM per device.

```python
import math
import jax
import jax.numpy as jnp
import numpy as np
from jax import lax

D = 2048
FF = 768
TOP = 8
EXPERTS = 16
TOKENS = 1024
BLK = 32
CAP = 32


def touch_ends(array, own_key, least, high):
    extent = array.shape
    place = [jax.random.randint(jax.random.fold_in(own_key, axis), (), 0, extent[axis]) for axis in range(len(extent))]
    array = array.at[tuple(place)].set(least)
    longest = extent.index(max(extent))
    place[longest] = (place[longest] + 1) % extent[longest]
    return array.at[tuple(place)].set(high)


def steps_of(own_key, shape, split, low, largest):
    def one(axis_at, parts):
        steps = jax.random.uniform(jax.random.fold_in(jax.random.fold_in(own_key, 6), axis_at), (parts,), jnp.float32, low / len(split), largest / len(split))
        return jnp.repeat(jnp.exp(steps), shape[axis_at] // parts).reshape((-1,) + (1,) * (len(shape) - axis_at - 1))

    level = one(*split[0])
    for cut in split[1:]:
        level = level * one(*cut)
    return level


def deal_out(own_key, own, number, rows, count, top, most, lean):
    order = jax.random.permutation(own_key, count)
    heavy_load, ordinary = shares(count, rows * top, most, lean, True), shares(count, rows * top, most, lean, False)
    places = jnp.arange(count)

    def named(tallies, rotation):
        used = int((tallies > 0).sum())
        fixed = max(1, used // 4)
        moved = fixed + (places - fixed + rotation * (used - fixed)) % max(1, count - fixed)
        return jnp.zeros((count,), jnp.int32).at[order[jnp.where(places < fixed, places, moved)]].set(jnp.asarray(tallies, jnp.int32))

    tallies = jnp.where(number % 4 == 0, named(heavy_load, number // 4), named(ordinary, number - number // 4 - 1))
    mixed = jax.random.permutation(jax.random.fold_in(own, 3), count)
    source_of, sink = mixed[0:count // 2 * 2:2], mixed[1:count // 2 * 2:2]
    margin = jnp.minimum(tallies[source_of] - 1, most - tallies[sink]) // 2
    margin = jnp.where((source_of == order[0]) | (sink == order[0]) | (tallies[sink] == 0), 0, jnp.maximum(margin, 0))
    moved = jax.random.randint(jax.random.fold_in(own, 4), (count // 2,), 0, 1 << 20) % (margin + 1)
    tallies = tallies.at[source_of].add(-moved).at[sink].add(moved)
    members = jnp.searchsorted(jnp.cumsum(tallies), jnp.arange(rows * top), side="right").astype(jnp.int32)
    table = members.reshape(top, rows).T
    table = table[jax.random.permutation(jax.random.fold_in(own, 1), rows)]
    rotation = jax.random.randint(jax.random.fold_in(own, 2), (rows, 1), 0, top)
    return jnp.take_along_axis(table, (jnp.arange(top)[None, :] + rotation) % top, axis=1)


def shares(amount, total, bound, lean, full):
    loads = [(1 << 20) // math.isqrt(rank ** lean) + 1 for rank in range(1, amount + 1)]
    largest = bound if full else min(bound, max(-(-total // amount), total * loads[0] // sum(loads)))
    least = 1 if total - largest >= amount - 1 else 0
    holding, surplus = [largest] + [least] * (amount - 1), total - largest - least * (amount - 1)
    while surplus > 0:
        movable = [i for i in range(1, amount) if holding[i] < largest] or [i for i in range(1, amount) if holding[i] < bound]
        mass, budget = sum([loads[i] for i in movable]), surplus
        for i in movable:
            addition = min(bound - holding[i], max(1, budget * loads[i] // mass), surplus)
            holding[i] = holding[i] + addition
            surplus = surplus - addition
    return np.array(holding)


def noise(rng, extent, deviation, limit, shards=(), held_as=jnp.bfloat16):
    entries = deviation * jax.random.normal(rng, extent, jnp.float32)
    if shards:
        entries = entries * steps_of(rng, extent, shards, -0.22, 0.18)
    return jnp.clip(entries, -limit, limit).astype(held_as)


def setup_inputs(seed: int = 0, part: int = 0) -> dict:
    keys = jax.random.split(jax.random.key(seed), 7)
    part_keys = jax.random.split(jax.random.fold_in(keys[6], part), 7)
    tokens = noise(part_keys[0], (TOKENS, D), 1.0, 6.0, ((0, 8),))
    expert_ids_keys = jax.random.split(jax.random.fold_in(part_keys[1], 1), TOKENS // BLK)
    expert_ids_turns = jax.random.permutation(jax.random.fold_in(part_keys[1], 3), TOKENS // BLK)
    expert_ids = jax.vmap(lambda own, number: deal_out(jax.random.fold_in(part_keys[1], 2), own, number, BLK, EXPERTS, TOP, CAP, 2))(expert_ids_keys, expert_ids_turns).reshape((TOKENS, TOP))
    gate_nums = touch_ends(jax.random.randint(part_keys[2], (TOKENS, TOP), 64, 1024), jax.random.fold_in(part_keys[2], 1), 64, 1023).astype(jnp.int32)
    w_gate = noise(keys[3], (EXPERTS, D, FF), D ** -0.5, 0.125, ((0, 8),))
    w_up = noise(keys[4], (EXPERTS, D, FF), D ** -0.5, 0.125, ((0, 8),))
    w_down = noise(keys[5], (EXPERTS, FF, D), FF ** -0.5, 0.21875, ((0, 8),))
    return {"tokens": tokens, "expert_ids": expert_ids, "gate_nums": gate_nums, "w_gate": w_gate, "w_up": w_up, "w_down": w_down}


denominator = 1024.0


def reference(tokens, expert_ids, gate_nums, w_gate, w_up, w_down):
    total = tokens.shape[0]
    most = CAP * (total // BLK)
    gates = gate_nums.astype(jnp.float32) / denominator

    def step(accum, expert):
        hit = expert_ids == expert
        weight = jnp.sum(jnp.where(hit, gates, jnp.zeros_like(gates)), axis=1)
        member = jnp.any(hit, axis=1)
        index = jnp.nonzero(member, size=most, fill_value=0)[0].astype(jnp.int32)
        valid = jnp.arange(most, dtype=jnp.int32) < jnp.sum(member.astype(jnp.int32))
        picked = tokens[index]
        gate = jnp.dot(picked, w_gate[expert], preferred_element_type=jnp.float32)
        up = jnp.dot(picked, w_up[expert], preferred_element_type=jnp.float32)
        hidden = (jax.nn.silu(gate) * up).astype(jnp.bfloat16)
        result = jnp.dot(hidden, w_down[expert], preferred_element_type=jnp.float32).astype(jnp.bfloat16)
        scale = jnp.where(valid, weight[index], jnp.zeros_like(weight[index]))
        accum = accum.at[index].add(scale[:, None] * result.astype(jnp.float32))
        return accum, None

    start = jnp.zeros((total, tokens.shape[1]), jnp.float32)
    accum, _ = lax.scan(step, start, jnp.arange(EXPERTS, dtype=jnp.int32))
    return accum.astype(jnp.bfloat16)
```

```python
import functools

import jax
import jax.numpy as jnp
from jax import lax
from jax.experimental import pallas as pl
from jax.experimental.pallas import tpu as pltpu
from jax.sharding import PartitionSpec as P

TOP = 8
BLOCKS = 4
TILE = 256


denominator = 1024.0


def packed_shards(tokens, expert_ids, gate_nums, w_gate, w_up, w_down):
    ways = lax.axis_size("ep")
    local = w_gate.shape[0]
    experts = local * ways
    width = tokens.shape[1]
    block_rows = tokens.shape[0] // BLOCKS
    slots = 2 * block_rows * TOP // experts
    gates = gate_nums.astype(jnp.float32) / denominator
    labels = jnp.arange(experts, dtype=jnp.int32)
    slot_ids = jnp.arange(slots, dtype=jnp.int32)

    def expert_work(received):
        gate = jnp.einsum("sxcd,xdf->sxcf", received, w_gate, preferred_element_type=jnp.float32)
        up = jnp.einsum("sxcd,xdf->sxcf", received, w_up, preferred_element_type=jnp.float32)
        hidden = (jax.nn.silu(gate) * up).astype(jnp.bfloat16)
        result = jnp.einsum("sxcf,xfd->sxcd", hidden, w_down, preferred_element_type=jnp.float32)
        return lax.all_to_all(
            result.astype(jnp.bfloat16), "ep", split_axis=0, concat_axis=0, tiled=True
        )

    places = []
    weights = []
    buffers = []
    for block in range(BLOCKS):
        lower = block * block_rows
        ids_blk = expert_ids[lower : lower + block_rows]
        gates_blk = gates[lower : lower + block_rows]
        rows_blk = tokens[lower : lower + block_rows]
        onehot = ids_blk[:, :, None] == labels[None, None, :]
        member = jnp.sum(onehot.astype(jnp.int32), axis=1)
        before = jnp.cumsum(member, axis=0) - member
        place = (before[:, :, None] == slot_ids[None, None, :]) & (member[:, :, None] > 0)
        weight = jnp.sum(jnp.where(onehot, gates_blk[:, :, None], 0.0), axis=1)
        packed = jnp.einsum(
            "bec,bd->ecd", place.astype(jnp.bfloat16), rows_blk, preferred_element_type=jnp.float32
        )
        buffers.append(packed.astype(jnp.bfloat16).reshape(ways, local, slots, width))
        places.append(place)
        weights.append(weight)
    backs = [
        expert_work(lax.all_to_all(buffers[block], "ep", split_axis=0, concat_axis=0, tiled=True))
        for block in range(BLOCKS)
    ]
    outputs = []
    for block in range(BLOCKS):
        back = backs[block].reshape(experts, slots, width)
        mixing = jnp.where(places[block], weights[block][:, :, None], 0.0)
        high = mixing.astype(jnp.bfloat16)
        low = (mixing - high.astype(jnp.float32)).astype(jnp.bfloat16)
        part_high = jnp.einsum("bec,ecd->bd", high, back, preferred_element_type=jnp.float32)
        part_low = jnp.einsum("bec,ecd->bd", low, back, preferred_element_type=jnp.float32)
        outputs.append(part_high + part_low)
    return jnp.concatenate(outputs, axis=0).astype(jnp.bfloat16)


def column(row):
    n = row.shape[1]
    square = lax.broadcasted_iota(jnp.int32, (n, n), 0) == lax.broadcasted_iota(
        jnp.int32, (n, n), 1
    )
    return jnp.sum(jnp.where(square, jnp.broadcast_to(row, (n, n)), 0.0), axis=1, keepdims=True)


def expert_kernel(a_ref, b_ref, scale_ref, wg_ref, wu_ref, wd_ref, oa_ref, ob_ref, x_ref, h_ref):
    rows = a_ref.shape[0]
    local, width, hidden = wg_ref.shape
    x_ref[:rows] = a_ref[...]
    x_ref[rows:] = b_ref[...]

    for e in range(local):

        @pl.loop(0, hidden // TILE)
        def _(f):
            cols = pl.ds(pl.multiple_of(f * TILE, TILE), TILE)
            x = x_ref[...]
            gate = jnp.dot(x, wg_ref[e, :, cols], preferred_element_type=jnp.float32)
            up = jnp.dot(x, wu_ref[e, :, cols], preferred_element_type=jnp.float32)
            h_ref[e, :, cols] = (jax.nn.silu(gate) * up).astype(jnp.bfloat16)

    scales = [
        jnp.concatenate([column(scale_ref[0, e : e + 1]), column(scale_ref[1, e : e + 1])], axis=0)
        for e in range(local)
    ]

    @pl.loop(0, width // TILE)
    def _(d):
        cols = pl.ds(pl.multiple_of(d * TILE, TILE), TILE)
        total = None
        for e in range(local):
            out = jnp.dot(h_ref[e], wd_ref[e, :, cols], preferred_element_type=jnp.float32)
            term = out.astype(jnp.bfloat16).astype(jnp.float32) * scales[e]
            total = term if total is None else total + term
        total = total.astype(jnp.bfloat16)
        oa_ref[:, cols] = total[:rows]
        ob_ref[:, cols] = total[rows:]


def expert_call(a, b, scale, w_gate, w_up, w_down):
    rows, width = a.shape
    local, _, hidden = w_gate.shape
    in_vmem = pl.BlockSpec(memory_space=pltpu.VMEM)
    held = [pltpu.with_memory_space_constraint(w, pltpu.VMEM) for w in (w_gate, w_up, w_down)]
    out = jax.ShapeDtypeStruct((rows, width), jnp.bfloat16)
    return pl.pallas_call(
        expert_kernel,
        out_shape=(out, out),
        in_specs=[in_vmem] * 6,
        out_specs=(in_vmem, in_vmem),
        scratch_shapes=[
            pltpu.VMEM((2 * rows, width), jnp.bfloat16),
            pltpu.VMEM((local, 2 * rows, hidden), jnp.bfloat16),
        ],
        cost_estimate=pl.CostEstimate(
            flops=2 * 2 * rows * local * width * hidden * 3,
            bytes_accessed=4 * rows * width * 2,
            transcendentals=2 * rows * local * hidden,
        ),
        compiler_params=pltpu.CompilerParams(vmem_limit_bytes=12 << 20),
    )(a, b, scale, *held)


def dense_shards(tokens, expert_ids, gate_nums, w_gate, w_up, w_down):
    ways = lax.axis_size("ep")
    local = w_gate.shape[0]
    rows = tokens.shape[0]
    planes = ways // 2
    me = lax.axis_index("ep")
    gates = gate_nums.astype(jnp.float32) / denominator
    labels = jnp.arange(local * ways, dtype=jnp.int32)
    hit = expert_ids.T[None, :, :] == labels[:, None, None]
    weight = jnp.sum(jnp.where(hit, gates.T[None, :, :], 0.0), axis=1)
    scales = lax.all_to_all(
        weight.reshape(ways, local, rows), "ep", split_axis=0, concat_axis=0, tiled=True
    )

    def swap(array, offset):
        return lax.ppermute(array, "ep", [(i, i ^ offset) for i in range(ways)])

    order = [1, 3, 2] if planes == 4 else list(range(1, planes))
    here = {0: tokens}
    there = {0: swap(tokens, 1)}
    for plane in order:
        here[plane] = swap(tokens, 2 * plane)
    for plane in order:
        there[plane] = swap(here[plane], 1)

    total = None
    for plane in order + [0]:
        source = me ^ (2 * plane)
        pair = jnp.stack(
            [
                lax.dynamic_index_in_dim(scales, source, keepdims=False),
                lax.dynamic_index_in_dim(scales, source ^ 1, keepdims=False),
            ]
        )
        own, other = expert_call(here[plane], there[plane], pair, w_gate, w_up, w_down)
        summed = own.astype(jnp.float32) + swap(other, 1).astype(jnp.float32)
        if plane:
            summed = swap(summed.astype(jnp.bfloat16), 2 * plane).astype(jnp.float32)
        total = summed if total is None else total + summed
    return total.astype(jnp.bfloat16)


def shards(tokens, expert_ids, gate_nums, w_gate, w_up, w_down):
    ways = lax.axis_size("ep")
    dense = 2 * TOP >= w_gate.shape[0] * ways and ways & (ways - 1) == 0 and ways > 1
    plan = dense_shards if dense else packed_shards
    return plan(tokens, expert_ids, gate_nums, w_gate, w_up, w_down)


def solution(mesh):
    placed = (
        P(("dp", "ep"), None),
        P(("dp", "ep"), None),
        P(("dp", "ep"), None),
        P("ep", None, None),
        P("ep", None, None),
        P("ep", None, None),
    )
    return jax.shard_map(
        shards, mesh=mesh, in_specs=placed, out_specs=P(("dp", "ep"), None), check_vma=False
    )
```
